32 devices in a mesh: groups: 2 (over x), dom: 16 (over z, y, core).
Axes of the slice: x: 2, y: 2, z: 4, core: 2. Of those that a mesh axis runs over, the one named last changes fastest.
Arguments:
- particles: bfloat16 [1024, 4096], P(('groups', 'dom')), parts along dimension 0, may hold values from -5 to 5
- dataset: bfloat16 [2048, 4096], P(('groups', 'dom')), parts along dimension 0, may hold values from -0.09375 to 0.09375
- labels: int32 [2048], P(('groups', 'dom')), parts along dimension 0, may hold values 0 or 1
- batch_index: int32 [512], P(('groups', 'dom')), parts along dimension 0, may hold values from 0 to 1023, as said below
Outputs:
- driving: float32 [1024, 4096], P(('groups', 'dom')), parts along dimension 0
- spreading: float32 [1024, 4096], P(('groups', 'dom')), parts along dimension 0
The draws below stay inside these ranges and needn't reach their ends.
There are 2 independent parts, one for each index of `groups`. The reference program is written for one: setup_inputs(seed, part) draws one part's arguments, and reference() takes and returns one part's arrays. A program takes and returns all parts, laid end to end along the dimension named above; each array names one. Nothing has to cross between parts.
Inputs may be any that keep to these rules, and one draw needn't show every extreme that they name: `batch_index`: entry b names a row of block b // 16 of the dataset, that is a row from (b // 16) * 64 to (b // 16 + 1) * 64 - 1; rows may repeat.
All inputs are finite; a program needn't handle non-finite values. No bound on the sum of `labels` on one device may be relied on, other than what follows from the above.
Results may differ from the reference program's by a relative error of at most 0.0003.
Values may be sent and summed in bfloat16 or wider, within the bound.
No kernel may reach another device: no remote copies, remote signals or barrier semaphores. Data moves between devices by JAX's collectives and lax.ppermute only.
A program may use at most 128 MiB of HBM per device.

```python
import jax
import jax.numpy as jnp
from jax import lax

D = 4096
BATCH_DEV = 16
DATA_DEV = 64
NP = 512
BATCH = 256
DATA = 1024


def draw_particles(key, part):
    key_centre = jax.random.fold_in(key, 11)
    key_radius = jax.random.fold_in(key, 12)
    key_noise = jax.random.fold_in(key, 13)
    key_directions = jax.random.fold_in(key, 14)
    key_latent = jax.random.fold_in(key, 15)
    centre = 0.5 * jnp.clip(jax.random.normal(key_centre, (D,), jnp.float32), -4.0, 4.0)
    radii = jnp.exp(jax.random.uniform(key_radius, (NP, 1), jnp.float32, jnp.log(0.1), jnp.log(0.3)))
    directions = jax.random.normal(key_directions, (8, D), jnp.float32) / jnp.sqrt(jnp.float32(D))
    spread = jnp.sqrt(jnp.float32(0.0390625 * D))
    noise = jnp.clip(jax.random.normal(key_noise, (NP, D), jnp.float32), -4.0, 4.0)
    latent = spread * jnp.clip(jax.random.normal(key_latent, (NP, 8), jnp.float32), -4.0, 4.0)
    placed = jnp.dot(latent, directions)
    field = centre[None, :] + placed + radii * noise
    return jnp.clip(field, -5.0, 5.0).astype(jnp.bfloat16)


def draw_batch_index(key, part):
    block = jnp.arange(BATCH, dtype=jnp.int32) // BATCH_DEV
    offset = jax.random.randint(jax.random.fold_in(key, 21), (BATCH,), 0, DATA_DEV, jnp.int32)
    return (block * DATA_DEV + offset).astype(jnp.int32)


def place_ends(drawn, stream_key, least, top_value):
    longest = drawn.shape.index(max(drawn.shape))
    spots = []
    for shift in (0, 1):
        where = [jax.random.randint(jax.random.fold_in(stream_key, axis), (), 0, length) for axis, length in enumerate(drawn.shape)]
        where[longest] = (where[longest] + shift) % drawn.shape[longest]
        spots.append(tuple(where))
    return drawn.at[spots[0]].set(least).at[spots[1]].set(top_value)


def level_of(stream_key, shape, cuts, low, top_value):
    level, own = 1.0, jax.random.fold_in(stream_key, 6)
    for dim, parts in cuts:
        steps = jnp.exp(jax.random.uniform(jax.random.fold_in(own, dim), (parts,), jnp.float32, low / len(cuts), top_value / len(cuts)))
        level = level * jnp.repeat(steps, shape[dim] // parts).reshape([-1 if axis == dim else 1 for axis in range(len(shape))])
    return level


def normal_values(stream_key, extent, width, bound, cuts=(), held_as=jnp.bfloat16):
    level = level_of(stream_key, extent, cuts, -0.22, 0.18) if cuts else 1.0
    array = jax.random.normal(stream_key, extent, jnp.float32) * width * level
    return jnp.minimum(jnp.maximum(array, -bound), bound).astype(held_as)


def setup_inputs(seed: int = 0, part: int = 0) -> dict:
    key_list = jax.random.split(jax.random.key(seed), 5)
    part_splits = jax.random.split(jax.random.fold_in(key_list[4], part), 5)
    return {
        "particles": draw_particles(jax.random.fold_in(jax.random.fold_in(key_list[4], part), 71), part),
        "dataset": normal_values(part_splits[1], (DATA, D), D ** -0.5, 0.09375, ((0, 16),)),
        "labels": place_ends((jax.random.randint(part_splits[2], (DATA,), 0, 2) < 1).astype(jnp.int32), jax.random.fold_in(part_splits[2], 1), 0, 1),
        "batch_index": draw_batch_index(jax.random.fold_in(jax.random.fold_in(key_list[4], part), 71), part),
    }


prior_precision = 1.0


def reference(particles, dataset, labels, batch_index):
    rows = jnp.take(dataset, batch_index, axis=0)
    targets = jnp.take(labels, batch_index).astype(jnp.float32)
    particles_f = particles.astype(jnp.float32)
    logits = lax.dot_general(particles, rows, (((1,), (1,)), ((), ())), preferred_element_type=jnp.float32)
    misfit = (targets[None, :] - jax.nn.sigmoid(logits)).astype(jnp.bfloat16)
    pulled = jnp.dot(misfit, rows, preferred_element_type=jnp.float32)
    scores = (-prior_precision * particles_f + (DATA / BATCH) * pulled).astype(jnp.bfloat16)
    squares = jnp.sum(particles_f * particles_f, axis=1)
    cross = lax.dot_general(particles, particles, (((1,), (1,)), ((), ())), preferred_element_type=jnp.float32)
    dist = squares[:, None] + squares[None, :] - 2.0 * cross
    kernel_scale = 0.25 * D
    kernel = jnp.exp(-dist / kernel_scale)
    kernel_b = kernel.astype(jnp.bfloat16)
    rowsum = jnp.sum(kernel, axis=1)
    drive = jnp.dot(kernel_b, scores, preferred_element_type=jnp.float32)
    pull = jnp.dot(kernel_b, particles, preferred_element_type=jnp.float32)
    driving = drive / NP
    spreading = (particles_f * rowsum[:, None] - pull) / NP
    return driving, spreading
```

```python
import functools

import jax
import jax.numpy as jnp
from jax import lax
from jax.experimental import pallas as pl
from jax.experimental.pallas import tpu as pltpu
from jax.sharding import PartitionSpec as P


prior_precision = 1.0


def pack_kernel(index_ref, label_ref, particles_ref, dataset_ref, bundle_ref):
    batch, own_rows = index_ref.shape[0], dataset_ref.shape[0]
    count = particles_ref.shape[0]
    bundle_ref[:count, :] = particles_ref[...]
    row = lax.broadcasted_iota(jnp.int32, (batch, own_rows), 0)
    col = lax.broadcasted_iota(jnp.int32, (batch, own_rows), 1)
    pick = jnp.zeros((batch, own_rows), jnp.float32)
    for b in range(batch):
        local = lax.rem(index_ref[b], own_rows)
        sign = (2 * label_ref[local] - 1).astype(jnp.float32)
        pick = jnp.where((row == b) & (col == local), sign, pick)
    picked = jnp.dot(
        pick.astype(jnp.bfloat16), dataset_ref[...], preferred_element_type=jnp.float32
    )
    bundle_ref[count:, :] = picked.astype(jnp.bfloat16)


def pack(particles, dataset, labels, batch_index):
    rows = particles.shape[0] + batch_index.shape[0]
    width = particles.shape[1]
    step = 1024
    return pl.pallas_call(
        pack_kernel,
        grid=(width // step,),
        out_shape=jax.ShapeDtypeStruct((rows, width), jnp.bfloat16),
        in_specs=[
            pl.BlockSpec(memory_space=pltpu.SMEM),
            pl.BlockSpec(memory_space=pltpu.SMEM),
            pl.BlockSpec((particles.shape[0], step), lambda k: (0, k)),
            pl.BlockSpec((dataset.shape[0], step), lambda k: (0, k)),
        ],
        out_specs=pl.BlockSpec((rows, step), lambda k: (0, k)),
    )(batch_index, labels, particles, dataset)


def to_row(column):
    n = column.shape[0]
    side = 128
    eye = lax.broadcasted_iota(jnp.int32, (side, side), 0) == lax.broadcasted_iota(
        jnp.int32, (side, side), 1
    )
    pieces = []
    for k in range(0, n, side):
        piece = jnp.broadcast_to(column[k : k + side, :], (side, side))
        pieces.append(jnp.sum(jnp.where(eye, piece, 0.0), axis=0, keepdims=True))
    return jnp.concatenate(pieces, axis=1)


def step_kernel(count, ratio, *refs):
    blocks = refs[:-6]
    driving_ref, spreading_ref, logits_ref, cross_ref, squares_ref, misfit_ref = refs[-6:]
    own = blocks[0]
    width = own.shape[1]
    total = count * len(blocks)
    contract_last = (((1,), (1,)), ((), ()))
    logits_ref[...] = jnp.zeros_like(logits_ref)
    cross_ref[...] = jnp.zeros_like(cross_ref)
    squares_ref[...] = jnp.zeros_like(squares_ref)

    def chunk_of(lanes, first, last):
        return jnp.concatenate([b[first:last, lanes] for b in blocks], axis=0)

    depth = 512

    @pl.loop(0, width // depth)
    def _(k):
        lanes = pl.ds(pl.multiple_of(k * depth, depth), depth)
        all_p = chunk_of(lanes, 0, count)
        all_r = chunk_of(lanes, count, own.shape[0])
        logits_ref[...] += lax.dot_general(
            all_p, all_r, contract_last, preferred_element_type=jnp.float32
        )
        cross_ref[...] += lax.dot_general(
            own[:count, lanes], all_p, contract_last, preferred_element_type=jnp.float32
        )
        all_f = all_p.astype(jnp.float32)
        square = all_f * all_f
        part = square[:, :128]
        for t in range(128, depth, 128):
            part += square[:, t : t + 128]
        squares_ref[...] += part

    misfit_ref[...] = (1.0 / (1.0 + jnp.exp(logits_ref[...]))).astype(jnp.bfloat16)
    squares = jnp.sum(squares_ref[...], axis=1, keepdims=True)
    kernel_scale = 0.25 * width
    dist = squares[:count, :] + to_row(squares) - 2.0 * cross_ref[...]
    kernel = jnp.exp(-dist / kernel_scale)
    kernel_b = kernel.astype(jnp.bfloat16)
    rowsum = jnp.sum(kernel, axis=1, keepdims=True)
    span = 256

    @pl.loop(0, width // span)
    def _(k):
        lanes = pl.ds(pl.multiple_of(k * span, span), span)
        all_p = chunk_of(lanes, 0, count)
        all_r = chunk_of(lanes, count, own.shape[0])
        pulled = jnp.dot(misfit_ref[...], all_r, preferred_element_type=jnp.float32)
        scores = (
            -prior_precision * all_p.astype(jnp.float32) + ratio * pulled
        ).astype(jnp.bfloat16)
        drive = jnp.dot(kernel_b, scores, preferred_element_type=jnp.float32)
        pull = jnp.dot(kernel_b, all_p, preferred_element_type=jnp.float32)
        own_f = own[:count, lanes].astype(jnp.float32)
        driving_ref[:, lanes] = drive / total
        spreading_ref[:, lanes] = (own_f * rowsum - pull) / total


def step(blocks, count, ratio):
    width = blocks[0].shape[1]
    batch = blocks[0].shape[0] - count
    total, total_batch = count * len(blocks), batch * len(blocks)
    out = jax.ShapeDtypeStruct((count, width), jnp.float32)
    return pl.pallas_call(
        functools.partial(step_kernel, count, ratio),
        out_shape=(out, out),
        in_specs=[pl.BlockSpec(memory_space=pltpu.VMEM)] * len(blocks),
        out_specs=(pl.BlockSpec(memory_space=pltpu.VMEM),) * 2,
        scratch_shapes=[
            pltpu.VMEM((total, total_batch), jnp.float32),
            pltpu.VMEM((count, total), jnp.float32),
            pltpu.VMEM((total, 128), jnp.float32),
            pltpu.VMEM((total, total_batch), jnp.bfloat16),
        ],
        compiler_params=pltpu.CompilerParams(vmem_limit_bytes=60 * 1024 * 1024),
    )(*blocks)


def rings(n):
    chips = n // 2
    order = list(range(0, chips, 2)) + list(range(1, chips, 2))[::-1]
    after = {q: order[(k + 1) % chips] for k, q in enumerate(order)}
    before = {q: p for p, q in after.items()}
    ring = [(2 * q, 2 * after[q]) for q in range(chips)]
    ring += [(2 * q + 1, 2 * before[q] + 1) for q in range(chips)]
    return ring, [(d, d ^ 1) for d in range(n)]


def per_device(n, particles, dataset, labels, batch_index):
    ring, swap = rings(n)
    chips = n // 2
    move = lambda x: lax.ppermute(x, "dom", ring)
    across = lambda x: lax.ppermute(x, "dom", swap)
    ratio = float(dataset.shape[0]) / float(batch_index.shape[0])
    first = pack(particles, dataset, labels, batch_index)
    second = across(first)
    blocks = [first, second]
    for _ in range((chips - 1) // 2):
        first, second = move(first), move(second)
        blocks += [first, second, across(first), across(second)]
    if chips % 2 == 0:
        first = move(first)
        blocks += [first, across(first)]
    return step(blocks, particles.shape[0], ratio)


def solution(mesh):
    rows = P(("groups", "dom"), None)
    flat = P(("groups", "dom"))
    return jax.shard_map(
        functools.partial(per_device, mesh.shape["dom"]),
        mesh=mesh,
        in_specs=(rows, rows, flat, flat),
        out_specs=(rows, rows),
        check_vma=False,
    )
```
